32 devices in a mesh: group: 4 (over y, core), peer: 8 (over z, x).
Axes of the slice: x: 2, y: 2, z: 4, core: 2. Of those that a mesh axis runs over, the one named last changes fastest.
Arguments:
- states: float32 [41, 1048576], P(None, ('group', 'peer')), may hold values from -6 to 6
- block_part: int32 [8192], P(('group', 'peer')), may hold values from 0 to 31, as said below
- tile_perm: int32 [8192, 128], P(('group', 'peer')), may hold values from 0 to 127, each once within a row
- half_volt: float32 [40], replicated, may hold values from -4 to 4
- steepness: float32 [40], replicated, may hold values from 0.5 to 4
- gate_rate: float32 [40], replicated, may hold values from 0.1 to 1
- conductance: float32 [40], replicated, may hold values from 0.005 to 0.08
- reversal: float32 [40], replicated, may hold values from -6 to 6
Outputs:
- regrouped: float32 [41, 1048576], P(None, ('group', 'peer'))
The draws below stay inside these ranges and needn't reach their ends.
Inputs may be any that keep to these rules, and one draw needn't show every extreme that they name: `block_part`: every partition holds exactly 256 blocks. Within each slab of 256 consecutive global blocks no partition holds more than 16 blocks; every slab has exactly 16 blocks of some partition, and every partition has exactly 16 blocks in some slab.
All inputs are finite; a program needn't handle non-finite values.
Results may differ from the reference program's by a relative error of at most 0.0001.
Values sent between devices are 32-bit elements; how exact they have to be, the bound alone decides.
A program may use at most 192 MiB of HBM per device.

```python
import math
import jax
import jax.numpy as jnp
from jax import lax

STATES = 41
NODE_BLK = 128
BLK_DEV = 256
SUBSTEPS = 1
GATES = 40
BLOCKS = 8192
NODES = 1048576


def draw_block_part(key, part):
    devices = BLOCKS // BLK_DEV
    mean_count = BLK_DEV // devices
    pair_count = devices // 2
    key_order = jax.random.fold_in(key, 11)
    key_amount = jax.random.fold_in(key, 12)
    key_shuffle = jax.random.fold_in(key, 13)
    ordering = jax.random.permutation(key_order, devices).astype(jnp.int32)
    amounts = jax.random.randint(key_amount, (pair_count,), -mean_count, mean_count + 1, dtype=jnp.int32)
    amounts = amounts.at[0].set(mean_count)
    row_ids = jnp.arange(devices, dtype=jnp.int32)
    pair_ids = jnp.arange(pair_count, dtype=jnp.int32)
    plus_cols = ordering[(row_ids[:, None] + 2 * pair_ids[None, :]) % devices]
    minus_cols = ordering[(row_ids[:, None] + 2 * pair_ids[None, :] + 1) % devices]
    row_grid = jnp.broadcast_to(row_ids[:, None], (devices, pair_count))
    amount_grid = jnp.broadcast_to(amounts[None, :], (devices, pair_count))
    counts = jnp.full((devices, devices), mean_count, jnp.int32)
    counts = counts.at[row_grid, plus_cols].add(amount_grid)
    counts = counts.at[row_grid, minus_cols].add(-amount_grid)
    running = jnp.cumsum(counts, axis=1, dtype=jnp.int32)
    position = jnp.arange(BLK_DEV, dtype=jnp.int32)
    labels = jnp.sum((running[:, None, :] <= position[None, :, None]).astype(jnp.int32), axis=2, dtype=jnp.int32)
    row_keys = jax.random.split(key_shuffle, devices)
    shuffled = jax.vmap(lambda row_key, row_vals: jax.random.permutation(row_key, row_vals))(row_keys, labels)
    return shuffled.reshape(-1).astype(jnp.int32)


def level_of(own_key, extent, cuts, low, largest):
    gain = 1.0
    for dim, parts in cuts:
        steps = jax.random.uniform(jax.random.fold_in(jax.random.fold_in(own_key, 6), dim), (parts,), jnp.float32, low / len(cuts), largest / len(cuts))
        gain = gain * jnp.repeat(jnp.exp(steps), extent[dim] // parts).reshape((-1,) + (1,) * (len(extent) - 1 - dim))
    return gain


def normal_values(stream_key, dims, width, reach, shards=(), kind=jnp.bfloat16):
    result = width * jax.random.normal(stream_key, dims, jnp.float32)
    if shards:
        result = result * level_of(stream_key, dims, shards, -0.22, 0.18)
    return jnp.clip(result, -reach, reach).astype(kind)


def setup_inputs(seed: int = 0) -> dict:
    key_list = jax.random.split(jax.random.key(seed), 9)
    return {
        "states": normal_values(key_list[0], (STATES, NODES), 1.0, 6.0, ((1, 32),), jnp.float32),
        "block_part": draw_block_part(jax.random.fold_in(key_list[8], 71), 0),
        "tile_perm": jax.vmap(lambda own: jax.random.permutation(own, NODE_BLK))(jax.random.split(key_list[2], BLOCKS)).reshape((BLOCKS, NODE_BLK)).astype(jnp.int32),
        "half_volt": normal_values(key_list[3], (GATES,), 1.0, 4.0, (), jnp.float32),
        "steepness": jnp.clip(jnp.exp(jax.random.uniform(key_list[4], (GATES,), jnp.float32, math.log(0.5), math.log(4.0))), 0.5, 4.0),
        "gate_rate": jnp.clip(jnp.exp(jax.random.uniform(key_list[5], (GATES,), jnp.float32, math.log(0.1), math.log(1.0))), 0.1, 1.0),
        "conductance": jnp.clip(jnp.exp(jax.random.uniform(key_list[6], (GATES,), jnp.float32, math.log(0.005), math.log(0.08))), 0.005, 0.08),
        "reversal": normal_values(key_list[7], (GATES,), 1.5, 6.0, (), jnp.float32),
    }


time_step = 0.25


def advance(state_rows, half_volt, steepness, gate_rate, conductance, reversal):
    voltage = state_rows[0:1]
    gate_vals = state_rows[1:]
    for substep in range(SUBSTEPS):
        steady = jax.nn.sigmoid((voltage - half_volt[:, None]) * steepness[:, None])
        damping = jnp.exp(-gate_rate[:, None] * (1.0 + jax.nn.sigmoid(voltage)))
        gate_vals = steady + (gate_vals - steady) * damping
        current = jnp.sum(conductance[:, None] * gate_vals * (voltage - reversal[:, None]), axis=0, keepdims=True)
        voltage = voltage - time_step * current
    return jnp.concatenate([voltage, gate_vals], axis=0)


def reference(states, block_part, tile_perm, half_volt, steepness, gate_rate, conductance, reversal):
    devices = BLOCKS // BLK_DEV
    span = BLK_DEV * NODE_BLK

    def one_part(index, acc):
        start = (index * span).astype(jnp.int32)
        piece = lax.dynamic_slice_in_dim(states, start, span, 1)
        done = advance(piece, half_volt, steepness, gate_rate, conductance, reversal)
        return lax.dynamic_update_slice_in_dim(acc, done, start, 1)

    advanced = lax.fori_loop(0, devices, one_part, jnp.zeros_like(states))
    ordering = jnp.argsort(block_part, stable=True).astype(jnp.int32)
    local_index = jnp.zeros((BLOCKS,), jnp.int32).at[ordering].set(jnp.arange(BLOCKS, dtype=jnp.int32))
    columns = (local_index[:, None] * NODE_BLK + tile_perm).reshape(-1).astype(jnp.int32)
    return jnp.take(advanced, columns, axis=1)
```

```python
import functools
import jax
import jax.numpy as jnp
import numpy as np
from jax import lax
from jax.experimental import pallas as pl
from jax.experimental.pallas import tpu as pltpu
from jax.sharding import PartitionSpec as P

time_step = 0.25
LANES = 128
ROWS = 8
MESH_ID = pl.DeviceIdType.MESH
VMEM_LIMIT = 67043328
SLOTS = 192
ORDERS = ((2, 1, 4, 0, 3), (0, 4, 3, 2, 1))


def submasks(bits):
    masks = [0]
    for bit in bits:
        masks = masks + [m | (1 << bit) for m in masks]
    return sorted(masks)


def stage_pairs(order, j):
    before, after = order[:j], order[j + 1 :]
    here = 1 << order[j]
    return [(a, b | here) for a in submasks(before) for b in submasks(after)]


def flip(d, mask):
    out = d
    bit = 0
    while (1 << bit) <= mask:
        if mask & (1 << bit):
            out = out + (1 - 2 * ((d // (1 << bit)) % 2)) * (1 << bit)
        bit += 1
    return out


def my_index(peers):
    return lax.axis_index("group") * peers + lax.axis_index("peer")


def counts_kernel(devices, peers, x_ref, out_ref, send_sem, recv_sem, local_sem):
    d = my_index(peers)
    barrier = pltpu.get_barrier_semaphore()
    for k in range(1, devices):
        to = (d + k) % devices
        pl.semaphore_signal(
            barrier, inc=1, device_id=(to // peers, to % peers), device_id_type=MESH_ID
        )
    pl.semaphore_wait(barrier, devices - 1)
    own = pltpu.make_async_copy(x_ref.at[0], out_ref.at[d], local_sem)
    own.start()
    for k in range(1, devices):
        to = (d + k) % devices
        pltpu.make_async_remote_copy(
            src_ref=x_ref.at[0], dst_ref=out_ref.at[d],
            send_sem=send_sem.at[k], recv_sem=recv_sem.at[k],
            device_id=(to // peers, to % peers), device_id_type=MESH_ID,
        ).start()
    own.wait()
    for k in range(1, devices):
        src = (d + devices - k) % devices
        pltpu.make_async_remote_copy(
            src_ref=x_ref.at[0], dst_ref=out_ref.at[src],
            send_sem=send_sem.at[k], recv_sem=recv_sem.at[k],
            device_id=(src // peers, src % peers), device_id_type=MESH_ID,
        ).wait()


def gather_counts(row, devices, peers):
    return pl.pallas_call(
        functools.partial(counts_kernel, devices, peers),
        out_shape=jax.ShapeDtypeStruct((devices, 1, LANES), jnp.int32),
        in_specs=[pl.BlockSpec(memory_space=pltpu.VMEM)],
        out_specs=pl.BlockSpec(memory_space=pltpu.VMEM),
        scratch_shapes=[
            pltpu.SemaphoreType.DMA((devices,)),
            pltpu.SemaphoreType.DMA((devices,)),
            pltpu.SemaphoreType.DMA,
        ],
        compiler_params=pltpu.CompilerParams(collective_id=0, has_side_effects=True),
    )(row)


def table_kernel(
    devices, peers, own_blocks, slots, c_ref, part_ref, tables_ref, final_ref, earlier
):
    d = my_index(peers)
    pool_size = own_blocks + len(ORDERS[0]) * slots
    run = jnp.int32(0)
    for s in range(devices):
        earlier[s] = run
        run = run + c_ref[s, 0, d]
    shape = (ROWS, LANES)
    flat = lax.broadcasted_iota(jnp.int32, shape, 0) * LANES + lax.broadcasted_iota(
        jnp.int32, shape, 1
    )
    tables_ref[...] = jnp.zeros_like(tables_ref)
    part = part_ref[...]
    sources = lax.broadcasted_iota(jnp.int32, (devices, own_blocks), 0)
    onehot = part == sources
    onehot_f = onehot.astype(jnp.float32)
    upper = (
        lax.broadcasted_iota(jnp.int32, (own_blocks, own_blocks), 0)
        < lax.broadcasted_iota(jnp.int32, (own_blocks, own_blocks), 1)
    ).astype(jnp.float32)
    rank = jnp.dot(onehot_f, upper, preferred_element_type=jnp.float32).astype(jnp.int32)
    near = lax.broadcasted_iota(jnp.int32, (devices, LANES), 0)
    final_ref[...] = jnp.zeros_like(final_ref)
    for o, order in enumerate(ORDERS):
        pos = {(0, m): earlier[flip(d, m)] for m in range(devices)}
        for j, bit in enumerate(order):
            pairs = stage_pairs(order, j)
            table = flat
            start = jnp.int32(0)
            shift = jnp.int32(0)
            for a, b in pairs:
                now = pos[(a, b)] - start
                table = table + jnp.where(flat >= start, now - shift, 0)
                shift = now
                start = start + c_ref[flip(d, b), 0, flip(d, a)]
            table = jnp.where(flat < start, table, 0)
            row = (o * len(order) + j) * 2
            tables_ref[row : row + 2, :] = table[0:2]
            fresh = {
                k: v for k, v in pos.items() if not (k[1] >> bit) & 1
            }
            partner = flip(d, 1 << bit)
            start = jnp.int32(own_blocks + j * slots)
            for a, b in pairs:
                fresh[(a | (1 << bit), b ^ (1 << bit))] = start
                start = start + c_ref[flip(partner, b), 0, flip(partner, a)]
            pos = fresh
        base = jnp.zeros((devices, LANES), jnp.int32)
        for a in range(devices):
            base = jnp.where(near == flip(d, a), pos[(a, 0)], base)
        whole = jnp.sum(jnp.where(onehot, base[:, 0:1] + rank, 0), axis=0, keepdims=True)
        whole = jnp.clip(whole, 0, pool_size - 1)
        final_ref[o : o + 1, :] = whole


def make_tables(counts, part, devices, peers, own_blocks, slots):
    return pl.pallas_call(
        functools.partial(table_kernel, devices, peers, own_blocks, slots),
        out_shape=(
            jax.ShapeDtypeStruct((24, LANES), jnp.int32),
            jax.ShapeDtypeStruct((8, own_blocks), jnp.int32),
        ),
        in_specs=[
            pl.BlockSpec(memory_space=pltpu.SMEM),
            pl.BlockSpec(memory_space=pltpu.VMEM),
        ],
        out_specs=(
            pl.BlockSpec(memory_space=pltpu.VMEM),
            pl.BlockSpec(memory_space=pltpu.VMEM),
        ),
        scratch_shapes=[pltpu.SMEM((devices,), jnp.int32)],
    )(counts, part)


def largest_load(counts, devices):
    ids = np.arange(devices)
    apart = ids[:, None] ^ ids[None, :]
    to_rows, from_rows = [], []
    for order in ORDERS:
        for j, bit in enumerate(order):
            before = sum(1 << b for b in order[:j])
            after = sum(1 << b for b in order[j + 1 :])
            here = 1 << bit
            to_rows.append(((apart & before) == 0) & ((apart & here) != 0))
            from_rows.append((apart & (here | after)) == 0)
    to_rows = jnp.asarray(np.concatenate(to_rows), jnp.bfloat16)
    from_rows = jnp.asarray(np.concatenate(from_rows), jnp.float32)
    part = jnp.dot(
        to_rows, counts.astype(jnp.bfloat16), preferred_element_type=jnp.float32
    )
    return jnp.max(jnp.sum(part * from_rows, axis=1)).astype(jnp.int32)


EVENTS = (
    (0, 0), (3, 0), (1, 0), (4, 0), (5, 0), (3, 1), (5, 1), (0, 1), (2, 0), (4, 1),
    (3, 2), (5, 2), (1, 1), (3, 3), (0, 2), (4, 2), (0, 3), (2, 1), (4, 3), (1, 2),
    (0, 4), (5, 3), (1, 3), (0, 5), (3, 4), (2, 2), (1, 4), (2, 3), (1, 5), (2, 4),
    (2, 5), (5, 4), (4, 4), (3, 5), (5, 5), (4, 5),
)
CHUNK_ORDER = (0, 0, 0, 1, 1, 1)
BUFFERS = {2: (0, 1), 1: (2, 3), 0: (4, 5), 4: (6,), 3: (7,)}


def exchange_kernel(
    peers, own_blocks, slots, unroll,
    tables, finals, params, states, out, out_row,
    pool, pool_row, landed, landed_row, packed, packed_row, ready, ready_row,
    send_sem, recv_sem, out_sem,
):
    d = my_index(peers)
    barrier = pltpu.get_barrier_semaphore()
    bits = sorted(ORDERS[0])
    for bit in bits:
        to = flip(d, 1 << bit)
        pl.semaphore_signal(
            barrier, inc=1, device_id=(to // peers, to % peers), device_id_type=MESH_ID
        )

    tiles = pool.shape[0]

    def advance_block(b):
        cols = pl.ds(pl.multiple_of(b * LANES, LANES), LANES)
        top = states[0:ROWS, cols]
        voltage = top[0:1, :]
        spread = jnp.broadcast_to(voltage, (ROWS, LANES))
        slow = -(1.0 + jax.nn.sigmoid(spread))

        def gates(vals, base, count):
            half, steep, rate, cond, rev = (
                params[k, base : base + count, :] for k in range(5)
            )
            v = spread[0:count]
            steady = jax.nn.sigmoid((v - half) * steep)
            damping = jnp.exp(rate * slow[0:count])
            new = steady + (vals - steady) * damping
            return new, cond * new * (v - rev)

        total = jnp.zeros((ROWS, LANES), jnp.float32)
        for t in range(1, tiles):
            new, term = gates(states[t * ROWS : (t + 1) * ROWS, cols], t * ROWS, ROWS)
            pool[t, b] = new
            total = total + term
        last = tiles * ROWS
        new_row, term_row = gates(states[last : last + 1, cols], last, 1)
        pool_row[pl.ds(b, 1), :] = new_row
        new, term = gates(top, 0, ROWS)
        total = total + term
        current = jnp.sum(total, axis=0, keepdims=True) + term_row
        moved = voltage - time_step * current
        first = lax.broadcasted_iota(jnp.int32, (ROWS, LANES), 0) == 0
        pool[0, b] = jnp.where(first, jnp.broadcast_to(moved, (ROWS, LANES)), new)

    def advance_loop(i, _):
        for u in range(4):
            advance_block(i * 4 + u)
        return 0

    lax.fori_loop(0, own_blocks // 4, advance_loop, 0)
    pl.semaphore_wait(barrier, len(bits))

    stages = len(bits)
    used = {}
    copies = {}
    outs = []
    turn = {bit: 0 for bit in bits}

    def arrive(c, j):
        copies[(c, j)].wait_recv()
        base = own_blocks + j * slots

        def move(i, _):
            for u in range(unroll):
                k = i * unroll + u
                if c < tiles:
                    pool[c, base + k] = landed[c, j, k]
            return 0

        if c < tiles:
            lax.fori_loop(0, slots // unroll, move, 0)
        else:
            pool_row[base : base + slots, :] = landed_row[j]

    for c, j in EVENTS:
        order = ORDERS[CHUNK_ORDER[c]]
        if j > 0:
            arrive(c, j - 1)
        if j < stages:
            bit = order[j]
            if c < tiles:
                names = BUFFERS[bit]
                buf = names[turn[bit] % len(names)]
                turn[bit] += 1
                if buf in used:
                    copies[used[buf]].wait_send()
                used[buf] = (c, j)
            row = (CHUNK_ORDER[c] * stages + j) * 2 * LANES

            def pack(i, _):
                for u in range(unroll):
                    k = i * unroll + u
                    at = tables[row + k]
                    if c < tiles:
                        packed[buf, k] = pool[c, at]
                    else:
                        packed_row[j, pl.ds(k, 1), :] = pool_row[pl.ds(at, 1), :]
                return 0

            lax.fori_loop(0, slots // unroll, pack, 0)
            to = flip(d, 1 << bit)
            copy = pltpu.make_async_remote_copy(
                src_ref=packed.at[buf] if c < tiles else packed_row.at[j],
                dst_ref=landed.at[c, j] if c < tiles else landed_row.at[j],
                send_sem=send_sem.at[c, j],
                recv_sem=recv_sem.at[c, j],
                device_id=(to // peers, to % peers),
                device_id_type=MESH_ID,
            )
            copy.start()
            copies[(c, j)] = copy
        else:
            if c < tiles and outs:
                outs.pop().wait()
            first = CHUNK_ORDER[c] * own_blocks

            def pick(i, _):
                for u in range(unroll):
                    k = i * unroll + u
                    at = finals[first + k]
                    if c < tiles:
                        ready[k] = pool[c, at]
                    else:
                        ready_row[pl.ds(k, 1), :] = pool_row[pl.ds(at, 1), :]
                return 0

            lax.fori_loop(0, own_blocks // unroll, pick, 0)
            if c < tiles:
                copy = pltpu.make_async_copy(ready, out.at[c], out_sem.at[0])
                copy.start()
                outs.append(copy)
            else:
                row_copy = pltpu.make_async_copy(ready_row, out_row, out_sem.at[1])
                row_copy.start()
    row_copy.wait()
    for copy in outs:
        copy.wait()
    last_use = set(used.values()) | {(tiles, j) for j in range(stages)}
    for key in sorted(last_use):
        copies[key].wait_send()


def exchange(tables, finals, params, states, peers, own_blocks, slots):
    tiles = states.shape[0] // ROWS
    stages = len(ORDERS[0])
    size = own_blocks + stages * slots
    f32 = jnp.float32
    return pl.pallas_call(
        functools.partial(exchange_kernel, peers, own_blocks, slots, 8),
        out_shape=(
            jax.ShapeDtypeStruct((tiles, own_blocks, ROWS, LANES), f32),
            jax.ShapeDtypeStruct((own_blocks, LANES), f32),
        ),
        in_specs=[
            pl.BlockSpec(memory_space=pltpu.SMEM),
            pl.BlockSpec(memory_space=pltpu.SMEM),
            pl.BlockSpec(memory_space=pltpu.VMEM),
            pl.BlockSpec(memory_space=pltpu.VMEM),
        ],
        out_specs=(
            pl.BlockSpec(memory_space=pl.ANY),
            pl.BlockSpec(memory_space=pl.ANY),
        ),
        scratch_shapes=[
            pltpu.VMEM((tiles, size, ROWS, LANES), f32),
            pltpu.VMEM((size, LANES), f32),
            pltpu.VMEM((tiles, stages, slots, ROWS, LANES), f32),
            pltpu.VMEM((stages, slots, LANES), f32),
            pltpu.VMEM((8, slots, ROWS, LANES), f32),
            pltpu.VMEM((stages, slots, LANES), f32),
            pltpu.VMEM((own_blocks, ROWS, LANES), f32),
            pltpu.VMEM((own_blocks, LANES), f32),
            pltpu.SemaphoreType.DMA((tiles + 1, stages)),
            pltpu.SemaphoreType.DMA((tiles + 1, stages)),
            pltpu.SemaphoreType.DMA((2,)),
        ],
        compiler_params=pltpu.CompilerParams(
            collective_id=1, has_side_effects=True, vmem_limit_bytes=VMEM_LIMIT
        ),
    )(tables, finals, params, states)


def place_kernel(tiles, blocks, got, got_row, perm, out):
    for group in range(blocks // ROWS):
        rows = slice(group * ROWS, (group + 1) * ROWS)
        turned = jnp.take_along_axis(
            got_row[rows, :], perm[rows, :], axis=1, mode="promise_in_bounds"
        )
        for u in range(ROWS):
            b = group * ROWS + u
            cols = slice(b * LANES, (b + 1) * LANES)
            where = jnp.broadcast_to(perm[b : b + 1, :], (ROWS, LANES))
            for t in range(tiles):
                out[t * ROWS : (t + 1) * ROWS, cols] = jnp.take_along_axis(
                    got[t, b], where, axis=1, mode="promise_in_bounds"
                )
            out[tiles * ROWS : tiles * ROWS + 1, cols] = turned[u : u + 1, :]


def place(got, got_row, perm, width, own_blocks):
    tiles = got.shape[0]
    step = 32
    return pl.pallas_call(
        functools.partial(place_kernel, tiles, step),
        grid=(own_blocks // step,),
        out_shape=jax.ShapeDtypeStruct((width, own_blocks * LANES), jnp.float32),
        in_specs=[
            pl.BlockSpec((tiles, step, ROWS, LANES), lambda i: (0, i, 0, 0)),
            pl.BlockSpec((step, LANES), lambda i: (i, 0)),
            pl.BlockSpec((step, LANES), lambda i: (i, 0)),
        ],
        out_specs=pl.BlockSpec((width, step * LANES), lambda i: (0, i)),
    )(got, got_row, perm)


def advance(state_rows, half_volt, steepness, gate_rate, conductance, reversal):
    voltage = state_rows[0:1]
    gate_vals = state_rows[1:]
    steady = jax.nn.sigmoid((voltage - half_volt[:, None]) * steepness[:, None])
    damping = jnp.exp(-gate_rate[:, None] * (1.0 + jax.nn.sigmoid(voltage)))
    gate_vals = steady + (gate_vals - steady) * damping
    current = jnp.sum(
        conductance[:, None] * gate_vals * (voltage - reversal[:, None]), axis=0, keepdims=True
    )
    voltage = voltage - time_step * current
    return jnp.concatenate([voltage, gate_vals], axis=0)


def general(counts_all, devices, states, block_part, tile_perm, *gate_params):
    d = lax.axis_index(("group", "peer"))
    local_blocks = block_part.shape[0]
    tile_width = tile_perm.shape[1]
    width = states.shape[0]
    capacity = 2 * local_blocks // devices
    partitions = jnp.arange(devices, dtype=jnp.int32)
    onehot = (block_part[:, None] == partitions[None, :]).astype(jnp.int32)
    before = (partitions < d).astype(jnp.int32)
    earlier = jnp.sum(counts_all * before[:, None], axis=0, dtype=jnp.int32)
    rank_in = jnp.sum(
        (jnp.cumsum(onehot, axis=0, dtype=jnp.int32) - onehot) * onehot, axis=1, dtype=jnp.int32
    )
    local_index = jnp.sum(onehot * earlier[None, :], axis=1, dtype=jnp.int32) + rank_in
    slot_index = block_part * capacity + rank_in
    requests = jnp.full((devices * capacity,), -1, jnp.int32).at[slot_index].set(local_index)
    requests = requests.reshape(devices, capacity)
    advanced = advance(states, *gate_params)
    advanced = advanced.reshape(width, local_blocks, tile_width)
    wanted = lax.all_to_all(requests, ("group", "peer"), split_axis=0, concat_axis=0, tiled=True)
    picked = jnp.maximum(wanted, 0).reshape(-1)
    served = jnp.take(advanced, picked, axis=1)
    arrived = lax.all_to_all(
        served.reshape(width, wanted.shape[0], wanted.shape[1], tile_width),
        ("group", "peer"), split_axis=1, concat_axis=1, tiled=True,
    )
    flat_cols = (slot_index[:, None] * tile_width + tile_perm).reshape(-1)
    return jnp.take(arrived.reshape(width, devices * capacity * tile_width), flat_cols, axis=1)


def on_device(devices, peers, states, block_part, tile_perm, *gate_params):
    own_blocks = block_part.shape[0]
    width = states.shape[0]
    partitions = jnp.arange(LANES, dtype=jnp.int32)
    counts = jnp.sum(
        (block_part[:, None] == partitions[None, :]).astype(jnp.int32), axis=0, dtype=jnp.int32
    )
    if devices != 1 << len(ORDERS[0]) or width % ROWS != 1:
        gathered = lax.all_gather(counts[:devices], ("group", "peer"))
        return general(gathered, devices, states, block_part, tile_perm, *gate_params)
    gathered = gather_counts(counts.reshape(1, 1, LANES), devices, peers)
    matrix = gathered[:, 0, :devices]
    fits = largest_load(matrix, devices) <= SLOTS
    tables, finals = make_tables(
        gathered, block_part.reshape(1, own_blocks), devices, peers, own_blocks, SLOTS
    )
    table_list = tables.reshape(-1)
    final_list = finals[0:2].reshape(-1)
    padded = jnp.stack([jnp.pad(p, (1, 0)) for p in gate_params])
    params = jnp.broadcast_to(padded[:, :, None], padded.shape + (LANES,))

    def fast():
        got, got_row = exchange(
            table_list, final_list, params, states, peers, own_blocks, SLOTS
        )
        return place(got, got_row, tile_perm, width, own_blocks)

    def slow():
        return general(matrix, devices, states, block_part, tile_perm, *gate_params)

    return lax.cond(fits, fast, slow)


def solution(mesh):
    both = P(("group", "peer"))
    return jax.shard_map(
        functools.partial(on_device, mesh.devices.size, mesh.shape["peer"]),
        mesh=mesh,
        in_specs=(P(None, ("group", "peer")), both, P(("group", "peer"), None)) + (P(),) * 5,
        out_specs=P(None, ("group", "peer")),
        check_vma=False,
    )
```

```python
import functools
import jax
import jax.numpy as jnp
import numpy as np
from jax import lax
from jax.experimental import pallas as pl
from jax.experimental.pallas import tpu as pltpu
from jax.sharding import PartitionSpec as P

time_step = 0.25
LANES = 128
ROWS = 8
MESH_ID = pl.DeviceIdType.MESH
VMEM_LIMIT = 67043328
SLOTS = (184, 208, 216, 200, 184)
ORDERS = ((2, 1, 4, 0, 3), (1, 2, 4, 0, 3), (0, 4, 3, 2, 1), (0, 4, 3, 1, 2))


def submasks(bits):
    masks = [0]
    for bit in bits:
        masks = masks + [m | (1 << bit) for m in masks]
    return sorted(masks)


def stage_pairs(order, j):
    before, after = order[:j], order[j + 1 :]
    here = 1 << order[j]
    return [(a, b | here) for a in submasks(before) for b in submasks(after)]


def flip(d, mask):
    out = d
    bit = 0
    while (1 << bit) <= mask:
        if mask & (1 << bit):
            out = out + (1 - 2 * ((d // (1 << bit)) % 2)) * (1 << bit)
        bit += 1
    return out


def my_index(peers):
    return lax.axis_index("group") * peers + lax.axis_index("peer")


def counts_kernel(devices, peers, x_ref, out_ref, send_sem, recv_sem, local_sem):
    d = my_index(peers)
    barrier = pltpu.get_barrier_semaphore()
    for k in range(1, devices):
        to = (d + k) % devices
        pl.semaphore_signal(
            barrier, inc=1, device_id=(to // peers, to % peers), device_id_type=MESH_ID
        )
    pl.semaphore_wait(barrier, devices - 1)
    own = pltpu.make_async_copy(x_ref.at[0], out_ref.at[d], local_sem)
    own.start()
    for k in range(1, devices):
        to = (d + k) % devices
        pltpu.make_async_remote_copy(
            src_ref=x_ref.at[0], dst_ref=out_ref.at[d],
            send_sem=send_sem.at[k], recv_sem=recv_sem.at[k],
            device_id=(to // peers, to % peers), device_id_type=MESH_ID,
        ).start()
    own.wait()
    for k in range(1, devices):
        src = (d + devices - k) % devices
        pltpu.make_async_remote_copy(
            src_ref=x_ref.at[0], dst_ref=out_ref.at[src],
            send_sem=send_sem.at[k], recv_sem=recv_sem.at[k],
            device_id=(src // peers, src % peers), device_id_type=MESH_ID,
        ).wait()


def gather_counts(row, devices, peers):
    return pl.pallas_call(
        functools.partial(counts_kernel, devices, peers),
        out_shape=jax.ShapeDtypeStruct((devices, 1, LANES), jnp.int32),
        in_specs=[pl.BlockSpec(memory_space=pltpu.VMEM)],
        out_specs=pl.BlockSpec(memory_space=pltpu.VMEM),
        scratch_shapes=[
            pltpu.SemaphoreType.DMA((devices,)),
            pltpu.SemaphoreType.DMA((devices,)),
            pltpu.SemaphoreType.DMA,
        ],
        compiler_params=pltpu.CompilerParams(collective_id=0, has_side_effects=True),
    )(row)


def table_kernel(
    devices, peers, own_blocks, slots, c_ref, part_ref, tables_ref, final_ref, earlier
):
    d = my_index(peers)
    pool_size = own_blocks + sum(slots)
    run = jnp.int32(0)
    for s in range(devices):
        earlier[s] = run
        run = run + c_ref[s, 0, d]
    shape = (ROWS, LANES)
    flat = lax.broadcasted_iota(jnp.int32, shape, 0) * LANES + lax.broadcasted_iota(
        jnp.int32, shape, 1
    )
    part = part_ref[...]
    sources = lax.broadcasted_iota(jnp.int32, (devices, own_blocks), 0)
    onehot = part == sources
    onehot_f = onehot.astype(jnp.float32)
    upper = (
        lax.broadcasted_iota(jnp.int32, (own_blocks, own_blocks), 0)
        < lax.broadcasted_iota(jnp.int32, (own_blocks, own_blocks), 1)
    ).astype(jnp.float32)
    rank = jnp.dot(onehot_f, upper, preferred_element_type=jnp.float32).astype(jnp.int32)
    near = lax.broadcasted_iota(jnp.int32, (devices, LANES), 0)
    final_ref[...] = jnp.zeros_like(final_ref)
    for o, order in enumerate(ORDERS):
        pos = {(0, m): earlier[flip(d, m)] for m in range(devices)}
        for j, bit in enumerate(order):
            pairs = stage_pairs(order, j)
            table = flat
            start = jnp.int32(0)
            shift = jnp.int32(0)
            for a, b in pairs:
                now = pos[(a, b)] - start
                table = table + jnp.where(flat >= start, now - shift, 0)
                shift = now
                start = start + c_ref[flip(d, b), 0, flip(d, a)]
            table = jnp.where(flat < start, table, 0)
            row = (o * len(order) + j) * 2
            tables_ref[row : row + 2, :] = table[0:2]
            fresh = {
                k: v for k, v in pos.items() if not (k[1] >> bit) & 1
            }
            partner = flip(d, 1 << bit)
            start = jnp.int32(own_blocks + sum(slots[:j]))
            for a, b in pairs:
                fresh[(a | (1 << bit), b ^ (1 << bit))] = start
                start = start + c_ref[flip(partner, b), 0, flip(partner, a)]
            pos = fresh
        base = jnp.zeros((devices, LANES), jnp.int32)
        for a in range(devices):
            base = jnp.where(near == flip(d, a), pos[(a, 0)], base)
        whole = jnp.sum(jnp.where(onehot, base[:, 0:1] + rank, 0), axis=0, keepdims=True)
        whole = jnp.clip(whole, 0, pool_size - 1)
        final_ref[o : o + 1, :] = whole


def make_tables(counts, part, devices, peers, own_blocks, slots):
    return pl.pallas_call(
        functools.partial(table_kernel, devices, peers, own_blocks, slots),
        out_shape=(
            jax.ShapeDtypeStruct((2 * len(ORDERS) * len(slots), LANES), jnp.int32),
            jax.ShapeDtypeStruct((8, own_blocks), jnp.int32),
        ),
        in_specs=[
            pl.BlockSpec(memory_space=pltpu.SMEM),
            pl.BlockSpec(memory_space=pltpu.VMEM),
        ],
        out_specs=(
            pl.BlockSpec(memory_space=pltpu.VMEM),
            pl.BlockSpec(memory_space=pltpu.VMEM),
        ),
        scratch_shapes=[pltpu.SMEM((devices,), jnp.int32)],
    )(counts, part)


def messages_fit(counts, devices):
    ids = np.arange(devices)
    apart = ids[:, None] ^ ids[None, :]
    to_rows, from_rows, room = [], [], []
    for order in ORDERS:
        for j, bit in enumerate(order):
            before = sum(1 << b for b in order[:j])
            after = sum(1 << b for b in order[j + 1 :])
            here = 1 << bit
            to_rows.append(((apart & before) == 0) & ((apart & here) != 0))
            from_rows.append((apart & (here | after)) == 0)
            room.append(np.full((devices,), SLOTS[j]))
    to_rows = jnp.asarray(np.concatenate(to_rows), jnp.bfloat16)
    from_rows = jnp.asarray(np.concatenate(from_rows), jnp.float32)
    part = jnp.dot(
        to_rows, counts.astype(jnp.bfloat16), preferred_element_type=jnp.float32
    )
    room = jnp.asarray(np.concatenate(room), jnp.float32)
    return jnp.max(jnp.sum(part * from_rows, axis=1) - room) <= 0.0


EVENTS = (
    (1, 0), (0, 0), (3, 0), (4, 0), (5, 0), (3, 1), (5, 1), (0, 1), (1, 1), (4, 1),
    (3, 2), (5, 2), (4, 2), (2, 0), (3, 3), (0, 2), (1, 2), (4, 3), (0, 3), (1, 3),
    (0, 4), (1, 4), (2, 1), (3, 4), (5, 3), (0, 5), (1, 5), (4, 4), (2, 2), (5, 4),
    (2, 3), (2, 4), (2, 5), (3, 5), (5, 5), (4, 5),
)
CHUNK_ORDER = (0, 1, 1, 2, 3, 2)
BUFFERS = {2: (0, 1), 1: (2, 3), 0: (4, 5), 4: (6,), 3: (7,)}


def exchange_kernel(
    peers, own_blocks, slots, unroll,
    tables, finals, params, states, out, out_row,
    pool, pool_row, landed, landed_row, packed, packed_row, ready, ready_row,
    send_sem, recv_sem, out_sem,
):
    d = my_index(peers)
    barrier = pltpu.get_barrier_semaphore()
    bits = sorted(ORDERS[0])
    for bit in bits:
        to = flip(d, 1 << bit)
        pl.semaphore_signal(
            barrier, inc=1, device_id=(to // peers, to % peers), device_id_type=MESH_ID
        )

    tiles = pool.shape[0]

    def advance_block(b):
        cols = pl.ds(pl.multiple_of(b * LANES, LANES), LANES)
        top = states[0:ROWS, cols]
        voltage = top[0:1, :]
        spread = jnp.broadcast_to(voltage, (ROWS, LANES))
        slow = -(1.0 + jax.nn.sigmoid(spread))

        def gates(vals, base, count):
            half, steep, rate, cond, rev = (
                params[k, base : base + count, :] for k in range(5)
            )
            v = spread[0:count]
            steady = jax.nn.sigmoid((v - half) * steep)
            damping = jnp.exp(rate * slow[0:count])
            new = steady + (vals - steady) * damping
            return new, cond * new * (v - rev)

        total = jnp.zeros((ROWS, LANES), jnp.float32)
        for t in range(1, tiles):
            new, term = gates(states[t * ROWS : (t + 1) * ROWS, cols], t * ROWS, ROWS)
            pool[t, b] = new
            total = total + term
        last = tiles * ROWS
        new_row, term_row = gates(states[last : last + 1, cols], last, 1)
        pool_row[pl.ds(b, 1), :] = new_row
        new, term = gates(top, 0, ROWS)
        total = total + term
        current = jnp.sum(total, axis=0, keepdims=True) + term_row
        moved = voltage - time_step * current
        first = lax.broadcasted_iota(jnp.int32, (ROWS, LANES), 0) == 0
        pool[0, b] = jnp.where(first, jnp.broadcast_to(moved, (ROWS, LANES)), new)

    def advance_loop(i, _):
        for u in range(4):
            advance_block(i * 4 + u)
        return 0

    lax.fori_loop(0, own_blocks // 4, advance_loop, 0)
    pl.semaphore_wait(barrier, len(bits))

    stages = len(bits)
    used = {}
    copies = {}
    outs = []
    turn = {bit: 0 for bit in bits}

    def arrive(c, j):
        copies[(c, j)].wait_recv()
        begin = sum(slots[:j])
        base = own_blocks + begin

        def move(i, _):
            for u in range(unroll):
                k = i * unroll + u
                if c < tiles:
                    pool[c, base + k] = landed[c, begin + k]
            return 0

        if c < tiles:
            lax.fori_loop(0, slots[j] // unroll, move, 0)
        else:
            pool_row[base : base + slots[j], :] = landed_row[begin : begin + slots[j], :]

    for c, j in EVENTS:
        order = ORDERS[CHUNK_ORDER[c]]
        if j > 0:
            arrive(c, j - 1)
        if j < stages:
            bit = order[j]
            if c < tiles:
                names = BUFFERS[bit]
                buf = names[turn[bit] % len(names)]
                turn[bit] += 1
                if buf in used:
                    copies[used[buf]].wait_send()
                used[buf] = (c, j)
            begin, room = sum(slots[:j]), slots[j]
            row = (CHUNK_ORDER[c] * stages + j) * 2 * LANES

            def pack(i, _):
                for u in range(unroll):
                    k = i * unroll + u
                    at = tables[row + k]
                    if c < tiles:
                        packed[buf, k] = pool[c, at]
                    else:
                        packed_row[pl.ds(begin + k, 1), :] = pool_row[pl.ds(at, 1), :]
                return 0

            lax.fori_loop(0, room // unroll, pack, 0)
            to = flip(d, 1 << bit)
            copy = pltpu.make_async_remote_copy(
                src_ref=packed.at[buf, pl.ds(0, room)]
                if c < tiles
                else packed_row.at[pl.ds(begin, room)],
                dst_ref=landed.at[c, pl.ds(begin, room)]
                if c < tiles
                else landed_row.at[pl.ds(begin, room)],
                send_sem=send_sem.at[c, j],
                recv_sem=recv_sem.at[c, j],
                device_id=(to // peers, to % peers),
                device_id_type=MESH_ID,
            )
            copy.start()
            copies[(c, j)] = copy
        else:
            if c < tiles and outs:
                outs.pop().wait()
            first = CHUNK_ORDER[c] * own_blocks

            def pick(i, _):
                for u in range(unroll):
                    k = i * unroll + u
                    at = finals[first + k]
                    if c < tiles:
                        ready[k] = pool[c, at]
                    else:
                        ready_row[pl.ds(k, 1), :] = pool_row[pl.ds(at, 1), :]
                return 0

            lax.fori_loop(0, own_blocks // unroll, pick, 0)
            if c < tiles:
                copy = pltpu.make_async_copy(ready, out.at[c], out_sem.at[0])
                copy.start()
                outs.append(copy)
            else:
                row_copy = pltpu.make_async_copy(ready_row, out_row, out_sem.at[1])
                row_copy.start()
    row_copy.wait()
    for copy in outs:
        copy.wait()
    last_use = set(used.values()) | {(tiles, j) for j in range(stages)}
    for key in sorted(last_use):
        copies[key].wait_send()


def exchange(tables, finals, params, states, peers, own_blocks, slots):
    tiles = states.shape[0] // ROWS
    stages = len(ORDERS[0])
    size = own_blocks + sum(slots)
    f32 = jnp.float32
    return pl.pallas_call(
        functools.partial(exchange_kernel, peers, own_blocks, slots, 8),
        out_shape=(
            jax.ShapeDtypeStruct((tiles, own_blocks, ROWS, LANES), f32),
            jax.ShapeDtypeStruct((own_blocks, LANES), f32),
        ),
        in_specs=[
            pl.BlockSpec(memory_space=pltpu.SMEM),
            pl.BlockSpec(memory_space=pltpu.SMEM),
            pl.BlockSpec(memory_space=pltpu.VMEM),
            pl.BlockSpec(memory_space=pltpu.VMEM),
        ],
        out_specs=(
            pl.BlockSpec(memory_space=pl.ANY),
            pl.BlockSpec(memory_space=pl.ANY),
        ),
        scratch_shapes=[
            pltpu.VMEM((tiles, size, ROWS, LANES), f32),
            pltpu.VMEM((size, LANES), f32),
            pltpu.VMEM((tiles, sum(slots), ROWS, LANES), f32),
            pltpu.VMEM((sum(slots), LANES), f32),
            pltpu.VMEM((1 + max(max(b) for b in BUFFERS.values()), max(slots), ROWS, LANES), f32),
            pltpu.VMEM((sum(slots), LANES), f32),
            pltpu.VMEM((own_blocks, ROWS, LANES), f32),
            pltpu.VMEM((own_blocks, LANES), f32),
            pltpu.SemaphoreType.DMA((tiles + 1, stages)),
            pltpu.SemaphoreType.DMA((tiles + 1, stages)),
            pltpu.SemaphoreType.DMA((2,)),
        ],
        compiler_params=pltpu.CompilerParams(
            collective_id=1, has_side_effects=True, vmem_limit_bytes=VMEM_LIMIT
        ),
    )(tables, finals, params, states)


def place_kernel(tiles, blocks, got, got_row, perm, out):
    for group in range(blocks // ROWS):
        rows = slice(group * ROWS, (group + 1) * ROWS)
        turned = jnp.take_along_axis(
            got_row[rows, :], perm[rows, :], axis=1, mode="promise_in_bounds"
        )
        for u in range(ROWS):
            b = group * ROWS + u
            cols = slice(b * LANES, (b + 1) * LANES)
            where = jnp.broadcast_to(perm[b : b + 1, :], (ROWS, LANES))
            for t in range(tiles):
                out[t * ROWS : (t + 1) * ROWS, cols] = jnp.take_along_axis(
                    got[t, b], where, axis=1, mode="promise_in_bounds"
                )
            out[tiles * ROWS : tiles * ROWS + 1, cols] = turned[u : u + 1, :]


def place(got, got_row, perm, width, own_blocks):
    tiles = got.shape[0]
    step = 32
    return pl.pallas_call(
        functools.partial(place_kernel, tiles, step),
        grid=(own_blocks // step,),
        out_shape=jax.ShapeDtypeStruct((width, own_blocks * LANES), jnp.float32),
        in_specs=[
            pl.BlockSpec((tiles, step, ROWS, LANES), lambda i: (0, i, 0, 0)),
            pl.BlockSpec((step, LANES), lambda i: (i, 0)),
            pl.BlockSpec((step, LANES), lambda i: (i, 0)),
        ],
        out_specs=pl.BlockSpec((width, step * LANES), lambda i: (0, i)),
    )(got, got_row, perm)


def advance(state_rows, half_volt, steepness, gate_rate, conductance, reversal):
    voltage = state_rows[0:1]
    gate_vals = state_rows[1:]
    steady = jax.nn.sigmoid((voltage - half_volt[:, None]) * steepness[:, None])
    damping = jnp.exp(-gate_rate[:, None] * (1.0 + jax.nn.sigmoid(voltage)))
    gate_vals = steady + (gate_vals - steady) * damping
    current = jnp.sum(
        conductance[:, None] * gate_vals * (voltage - reversal[:, None]), axis=0, keepdims=True
    )
    voltage = voltage - time_step * current
    return jnp.concatenate([voltage, gate_vals], axis=0)


def general(counts_all, devices, states, block_part, tile_perm, *gate_params):
    d = lax.axis_index(("group", "peer"))
    local_blocks = block_part.shape[0]
    tile_width = tile_perm.shape[1]
    width = states.shape[0]
    capacity = 2 * local_blocks // devices
    partitions = jnp.arange(devices, dtype=jnp.int32)
    onehot = (block_part[:, None] == partitions[None, :]).astype(jnp.int32)
    before = (partitions < d).astype(jnp.int32)
    earlier = jnp.sum(counts_all * before[:, None], axis=0, dtype=jnp.int32)
    rank_in = jnp.sum(
        (jnp.cumsum(onehot, axis=0, dtype=jnp.int32) - onehot) * onehot, axis=1, dtype=jnp.int32
    )
    local_index = jnp.sum(onehot * earlier[None, :], axis=1, dtype=jnp.int32) + rank_in
    slot_index = block_part * capacity + rank_in
    requests = jnp.full((devices * capacity,), -1, jnp.int32).at[slot_index].set(local_index)
    requests = requests.reshape(devices, capacity)
    advanced = advance(states, *gate_params)
    advanced = advanced.reshape(width, local_blocks, tile_width)
    wanted = lax.all_to_all(requests, ("group", "peer"), split_axis=0, concat_axis=0, tiled=True)
    picked = jnp.maximum(wanted, 0).reshape(-1)
    served = jnp.take(advanced, picked, axis=1)
    arrived = lax.all_to_all(
        served.reshape(width, wanted.shape[0], wanted.shape[1], tile_width),
        ("group", "peer"), split_axis=1, concat_axis=1, tiled=True,
    )
    flat_cols = (slot_index[:, None] * tile_width + tile_perm).reshape(-1)
    return jnp.take(arrived.reshape(width, devices * capacity * tile_width), flat_cols, axis=1)


def on_device(devices, peers, states, block_part, tile_perm, *gate_params):
    own_blocks = block_part.shape[0]
    width = states.shape[0]
    partitions = jnp.arange(LANES, dtype=jnp.int32)
    counts = jnp.sum(
        (block_part[:, None] == partitions[None, :]).astype(jnp.int32), axis=0, dtype=jnp.int32
    )
    if devices != 1 << len(ORDERS[0]) or width % ROWS != 1:
        gathered = lax.all_gather(counts[:devices], ("group", "peer"))
        return general(gathered, devices, states, block_part, tile_perm, *gate_params)
    gathered = gather_counts(counts.reshape(1, 1, LANES), devices, peers)
    matrix = gathered[:, 0, :devices]
    fits = messages_fit(matrix, devices)
    tables, finals = make_tables(
        gathered, block_part.reshape(1, own_blocks), devices, peers, own_blocks, SLOTS
    )
    table_list = tables.reshape(-1)
    final_list = finals[0 : len(ORDERS)].reshape(-1)
    padded = jnp.stack([jnp.pad(p, (1, 0)) for p in gate_params])
    params = jnp.broadcast_to(padded[:, :, None], padded.shape + (LANES,))

    def fast():
        got, got_row = exchange(
            table_list, final_list, params, states, peers, own_blocks, SLOTS
        )
        return place(got, got_row, tile_perm, width, own_blocks)

    def slow():
        return general(matrix, devices, states, block_part, tile_perm, *gate_params)

    return lax.cond(fits, fast, slow)


def solution(mesh):
    both = P(("group", "peer"))
    return jax.shard_map(
        functools.partial(on_device, mesh.devices.size, mesh.shape["peer"]),
        mesh=mesh,
        in_specs=(P(None, ("group", "peer")), both, P(("group", "peer"), None)) + (P(),) * 5,
        out_specs=P(None, ("group", "peer")),
        check_vma=False,
    )
```
